32 devices in a mesh: dp: 8 (over z, y), mp: 4 (over x, core).
Axes of the slice: x: 2, y: 2, z: 4, core: 2. Of those that a mesh axis runs over, the one named last changes fastest.
Arguments:
- block_input: bfloat16 [16, 1024, 1536], P('dp'), may hold values from -6 to 6
- zx_weight: bfloat16 [2, 2, 1536, 3072], P(None, None, 'dp', 'mp'), may hold values from -0.15625 to 0.15625
- bc_weight: bfloat16 [2, 1536, 256], P(None, 'dp'), may hold values from -0.15625 to 0.15625
- dt_weight: bfloat16 [2, 1536, 48], P(None, 'dp', 'mp'), may hold values from -0.15625 to 0.15625
- out_weight: bfloat16 [2, 3072, 1536], P(None, 'mp', 'dp'), may hold values from -0.109375 to 0.109375
- norm_gain: float32 [2, 1536], replicated, may hold values from 0.1 to 1.9
- inner_conv: float32 [2, 4, 3072], P(None, None, 'mp'), may hold values from -3 to 3
- inner_conv_bias: float32 [2, 3072], P(None, 'mp'), may hold values from -3 to 3
- state_conv: float32 [2, 4, 256], replicated, may hold values from -3 to 3
- state_conv_bias: float32 [2, 256], replicated, may hold values from -3 to 3
- dt_bias: float32 [2, 48], P(None, 'mp'), may hold values from -5 to -1
- a_log: float32 [2, 48], P(None, 'mp'), may hold values from 0 to 2.5
- d_skip: float32 [2, 48], P(None, 'mp'), may hold values from 0.5 to 2
- gated_gain: float32 [2, 3072], P(None, 'mp'), may hold values from 0.1 to 1.9
- cotangent: bfloat16 [16, 1024, 1536], P('dp'), may hold values from -6 to 6
Outputs:
- block_output: bfloat16 [16, 1024, 1536], P('dp')
- input_grad: float32 [16, 1024, 1536], P('dp')
- zx_grad: float32 [2, 2, 1536, 3072], P(None, None, 'dp', 'mp')
- bc_grad: float32 [2, 1536, 256], P(None, 'dp')
- dt_grad: float32 [2, 1536, 48], P(None, 'dp', 'mp')
- out_grad: float32 [2, 3072, 1536], P(None, 'mp', 'dp')
- norm_gain_grad: float32 [2, 1536], replicated
- inner_conv_grad: float32 [2, 4, 3072], P(None, None, 'mp')
- inner_conv_bias_grad: float32 [2, 3072], P(None, 'mp')
- state_conv_grad: float32 [2, 4, 256], replicated
- state_conv_bias_grad: float32 [2, 256], replicated
- dt_bias_grad: float32 [2, 48], P(None, 'mp')
- a_log_grad: float32 [2, 48], P(None, 'mp')
- d_skip_grad: float32 [2, 48], P(None, 'mp')
- gated_gain_grad: float32 [2, 3072], P(None, 'mp')
The draws below stay inside these ranges and needn't reach their ends.
All inputs are finite; a program needn't handle non-finite values.
Results may differ from the reference program's by a relative error of at most 0.035.
Values may be sent and summed in bfloat16 or wider, within the bound.
A program may use at most 320 MiB of HBM per device.

```python
import jax
import jax.numpy as jnp
from jax import lax

D = 1536
HEADS = 48
STATE = 128
KW = 4
SCAN_BLOCK = 256
LAYERS = 2
LEN = 1024
INNER = 3072
BATCH = 16
N_MP = 4


def block_levels(rng, shape, cuts, least, largest):
    factor_of = 1.0
    for dim, shards_of in cuts:
        steps = jax.random.uniform(jax.random.fold_in(jax.random.fold_in(rng, 6), dim), (shards_of,), jnp.float32, least / len(cuts), largest / len(cuts))
        factor_of = factor_of * jnp.repeat(jnp.exp(steps), shape[dim] // shards_of).reshape((-1,) + (1,) * (len(shape) - 1 - dim))
    return factor_of


def bell_draw(key, dims, scale, limit, split=(), held_as=jnp.bfloat16):
    array = scale * jax.random.normal(key, dims, jnp.float32)
    if split:
        array = array * block_levels(key, dims, split, -0.22, 0.18)
    return jnp.clip(array, -limit, limit).astype(held_as)


def setup_inputs(seed: int = 0) -> dict:
    splits = jax.random.split(jax.random.key(seed), 16)
    return {
        "block_input": bell_draw(splits[0], (BATCH, LEN, D), 1.0, 6.0, ((0, 8),)),
        "zx_weight": bell_draw(splits[1], (LAYERS, 2, D, INNER), D ** -0.5, 0.15625, ((2, 8), (3, 4))),
        "bc_weight": bell_draw(splits[2], (LAYERS, D, 2 * STATE), D ** -0.5, 0.15625, ((1, 8),)),
        "dt_weight": bell_draw(splits[3], (LAYERS, D, HEADS), D ** -0.5, 0.15625, ((1, 8), (2, 4))),
        "out_weight": bell_draw(splits[4], (LAYERS, INNER, D), INNER ** -0.5, 0.109375, ((1, 4), (2, 8))),
        "norm_gain": jnp.clip(1.0 + 0.18 * jax.random.normal(splits[5], (LAYERS, D), jnp.float32), 0.1, 1.9),
        "inner_conv": bell_draw(splits[6], (LAYERS, KW, INNER), KW ** -0.5, 3.0, ((2, 4),), jnp.float32),
        "inner_conv_bias": bell_draw(splits[7], (LAYERS, INNER), 0.5, 3.0, ((1, 4),), jnp.float32),
        "state_conv": bell_draw(splits[8], (LAYERS, KW, 2 * STATE), KW ** -0.5, 3.0, (), jnp.float32),
        "state_conv_bias": bell_draw(splits[9], (LAYERS, 2 * STATE), 0.5, 3.0, (), jnp.float32),
        "dt_bias": jnp.clip(-5.0 + 4.0 * jax.random.uniform(splits[10], (LAYERS, HEADS), jnp.float32) ** block_levels(splits[10], (LAYERS, HEADS), ((1, 4),), -0.2, 0.2), -5.0, -1.0),
        "a_log": jnp.clip(2.5 * jax.random.uniform(splits[11], (LAYERS, HEADS), jnp.float32) ** block_levels(splits[11], (LAYERS, HEADS), ((1, 4),), -0.2, 0.2), 0.0, 2.5),
        "d_skip": jnp.clip(0.5 + 1.5 * jax.random.uniform(splits[12], (LAYERS, HEADS), jnp.float32) ** block_levels(splits[12], (LAYERS, HEADS), ((1, 4),), -0.2, 0.2), 0.5, 2.0),
        "gated_gain": jnp.clip(1.0 + 0.18 * jax.random.normal(splits[13], (LAYERS, INNER), jnp.float32), 0.1, 1.9),
        "cotangent": bell_draw(splits[14], (BATCH, LEN, D), 1.0, 6.0, ((0, 8),)),
    }


EPS = 1e-05
HIGH = lax.Precision.HIGHEST

@jax.custom_vjp
def low(v):
    return lax.optimization_barrier(v.astype(jnp.bfloat16)).astype(jnp.float32)

@jax.custom_vjp
def low_back(v):
    return v

def low_keep(v):
    return (low(v), None)

def low_pass(kept, grad):
    return (grad,)

def back_keep(v):
    return (v, None)

def back_low(kept, grad):
    return (low(grad),)
low.defvjp(low_keep, low_pass)
low_back.defvjp(back_keep, back_low)

def causal_conv(values, kernel, offset):
    length = values.shape[0]
    taps = kernel.shape[0]
    padded = jnp.pad(values, ((taps - 1, 0), (0, 0)))
    running = jnp.zeros_like(values) + offset[None, :]
    for tap_at in range(taps):
        running = running + kernel[tap_at][None, :] * padded[tap_at:tap_at + length]
    return running

def block_scan(inner_vals, step_vals, decay_rates, key_rows, query_rows, block_len):
    length, head_count, head_width = inner_vals.shape
    block_count = length // block_len
    state_size = key_rows.shape[1]
    inner_blocks = inner_vals.reshape(block_count, block_len, head_count, head_width)
    step_blocks = step_vals.reshape(block_count, block_len, head_count)
    key_blocks = key_rows.reshape(block_count, block_len, state_size)
    query_blocks = query_rows.reshape(block_count, block_len, state_size)
    lower_mask = jnp.tril(jnp.ones((block_len, block_len), jnp.float32))[:, :, None]

    def one_block(carried, pieces):
        values, deltas, keys_here, queries_here = pieces
        log_decay = jnp.cumsum(deltas * decay_rates[None, :], axis=0)
        scores = jnp.dot(queries_here, keys_here.T, precision=HIGH)
        gaps = log_decay[:, None, :] - log_decay[None, :, :]
        decays = lower_mask * jnp.exp(jnp.where(lower_mask > 0, gaps, 0.0))
        mixing = scores[:, :, None] * decays * deltas[None, :, :]
        within = jnp.einsum('tsh,shp->thp', mixing, values, precision=HIGH)
        from_state = jnp.exp(log_decay)[:, :, None] * jnp.einsum('tn,hpn->thp', queries_here, carried, precision=HIGH)
        final_log = log_decay[-1]
        weights_end = jnp.exp(final_log[None, :] - log_decay) * deltas
        update = jnp.einsum('sh,shp,sn->hpn', weights_end, values, keys_here, precision=HIGH)
        return (jnp.exp(final_log)[:, None, None] * carried + update, within + from_state)
    start = jnp.zeros((head_count, head_width, state_size), jnp.float32)
    ended, outputs = lax.scan(jax.checkpoint(one_block), start, (inner_blocks, step_blocks, key_blocks, query_blocks))
    return outputs.reshape(length, head_count, head_width)

def ssd_mixer(gate_part, inner_part, state_part, step_raw, inner_conv, inner_conv_bias, state_conv, state_conv_bias, dt_bias, a_log, d_skip):
    length = gate_part.shape[0]
    head_count = dt_bias.shape[0]
    inner_act = jax.nn.silu(causal_conv(inner_part, inner_conv, inner_conv_bias))
    state_act = jax.nn.silu(causal_conv(state_part, state_conv, state_conv_bias))
    half_state = state_act.shape[1] // 2
    step_pos = jax.nn.softplus(step_raw + dt_bias[None, :])
    decay_rates = -jnp.exp(a_log)
    shaped = inner_act.reshape(length, head_count, -1)
    scanned = block_scan(shaped, step_pos, decay_rates, state_act[:, :half_state], state_act[:, half_state:], SCAN_BLOCK)
    mixed_out = scanned + d_skip[None, :, None] * shaped
    return mixed_out.reshape(length, -1) * jax.nn.silu(gate_part)

def layer_forward(hidden, params):
    zx_weight, bc_weight, dt_weight, out_weight, norm_gain, inner_conv, inner_conv_bias, state_conv, state_conv_bias, dt_bias, a_log, d_skip, gated_gain = params
    length = hidden.shape[0]
    root_row = lax.rsqrt(lax.optimization_barrier(jnp.mean(hidden * hidden, axis=-1)) + EPS)
    normed = low(hidden * root_row[:, None] * norm_gain[None, :])
    both_parts = low_back(jnp.einsum('td,kdi->tki', normed, zx_weight, precision=HIGH))
    state_part = jnp.dot(normed, bc_weight, precision=HIGH)
    step_raw = low_back(jnp.dot(normed, dt_weight, precision=HIGH))
    gated_val = ssd_mixer(both_parts[:, 0], both_parts[:, 1], state_part, step_raw, inner_conv, inner_conv_bias, state_conv, state_conv_bias, dt_bias, a_log, d_skip)
    scale_row = lax.rsqrt(lax.optimization_barrier(jnp.mean(gated_val * gated_val, axis=-1)) + EPS)
    weighted = low(gated_val * gated_gain[None, :])
    pieces = jnp.einsum('tgi,gid->gtd', weighted.reshape(length, N_MP, -1), out_weight.reshape(N_MP, -1, out_weight.shape[1]), precision=HIGH)
    summed = low_back(lax.optimization_barrier(jnp.sum(low(pieces), axis=0)))
    return hidden + scale_row[:, None] * summed

def reference(block_input, zx_weight, bc_weight, dt_weight, out_weight, norm_gain, inner_conv, inner_conv_bias, state_conv, state_conv_bias, dt_bias, a_log, d_skip, gated_gain, cotangent):
    params = tuple((array_in.astype(jnp.float32) for array_in in (zx_weight, bc_weight, dt_weight, out_weight, norm_gain, inner_conv, inner_conv_bias, state_conv, state_conv_bias, dt_bias, a_log, d_skip, gated_gain)))

    def forward(sequence, weights):
        hidden = sequence
        for layer_at in range(LAYERS):
            hidden = layer_forward(hidden, tuple((item[layer_at] for item in weights)))
        return hidden

    def per_sequence(totals, pair_in):
        sequence, tangent = pair_in
        result, pullback = jax.vjp(forward, sequence, params)
        seq_grad, weight_grads = pullback(tangent)
        totals = jax.tree.map(lambda earlier, latest: earlier + latest, totals, weight_grads)
        return (totals, (result.astype(jnp.bfloat16), seq_grad))
    zero_grads = jax.tree.map(jnp.zeros_like, params)
    totals, (outputs, input_grads) = lax.scan(per_sequence, zero_grads, (block_input.astype(jnp.float32), cotangent.astype(jnp.float32)))
    return (outputs, input_grads, totals[0], totals[1], totals[2], totals[3], totals[4], totals[5], totals[6], totals[7], totals[8], totals[9], totals[10], totals[11], totals[12])
```

```python
import functools

import jax
import jax.numpy as jnp
from jax import lax
from jax.experimental import pallas as pl
from jax.experimental.pallas import tpu as pltpu
from jax.sharding import PartitionSpec as P

EPS = 1e-05
HIGH = lax.Precision.HIGHEST
CHUNK = 128
TAPS = 4
F32 = jnp.float32
BF16 = jnp.bfloat16


def dot_nn(a, b):
    return lax.dot_general(a, b, (((1,), (0,)), ((), ())), preferred_element_type=F32)


def dot_nt(a, b):
    return lax.dot_general(a, b, (((1,), (1,)), ((), ())), preferred_element_type=F32)


def dot_tn(a, b):
    return lax.dot_general(a, b, (((0,), (0,)), ((), ())), preferred_element_type=F32)


def sigmoid(v):
    return 0.5 * jnp.tanh(0.5 * v) + 0.5


def softplus(v):
    return jnp.maximum(v, 0.0) + jnp.log1p(jnp.exp(-jnp.abs(v)))


def lanes_of(shape):
    return lax.broadcasted_iota(jnp.int32, shape, 1)


def rows_of(shape):
    return lax.broadcasted_iota(jnp.int32, shape, 0)


def shifted_right(now, before, by):
    merged = jnp.where(lanes_of(now.shape) >= CHUNK - by, before, now)
    return pltpu.roll(merged, by, 1)


def shifted_left(now, after, by):
    merged = jnp.where(lanes_of(now.shape) < by, after, now)
    return pltpu.roll(merged, CHUNK - by, 1)


def decay_pieces(raw, bias, rate):
    step = softplus(raw + bias)
    upper = (rows_of((CHUNK, CHUNK)) <= lanes_of((CHUNK, CHUNK))).astype(F32)
    cum = lax.dot_general(
        step * rate, upper, (((1,), (0,)), ((), ())), precision=HIGH, preferred_element_type=F32
    )
    return step, cum


def transposed(a):
    rows = a.shape[0]
    padded = jnp.concatenate([a, jnp.zeros((CHUNK - rows, CHUNK), F32)], axis=0)
    return jnp.transpose(padded)


def forward_body(dims, z_ref, conv_ref, head_ref, row_ref, w_ref, sq_ref, y_ref, s_ref, act, tail, state, wide):
    inner, heads, width, states = dims
    chans = inner + 2 * states
    at = pl.program_id(0)

    @pl.when(at == 0)
    def _():
        tail[...] = jnp.zeros_like(tail)
        state[...] = jnp.zeros_like(state)
        for which in range(TAPS + 1):
            wide[which] = jnp.broadcast_to(conv_ref[:, which : which + 1], (chans, CHUNK))

    for row in range(0, chans, width):
        span = slice(row, row + width)
        now = z_ref[inner + row : inner + row + width, :].astype(F32)
        before = tail[span, :].astype(F32)
        conv = wide[TAPS, span, :] + wide[TAPS - 1, span, :] * now
        for by in range(1, TAPS):
            conv = conv + wide[TAPS - 1 - by, span, :] * shifted_right(now, before, by)
        act[span, :] = conv * sigmoid(conv)
    tail[...] = z_ref[inner : inner + chans, :]

    step, cum = decay_pieces(
        z_ref[inner + chans :, :].astype(F32), head_ref[:, 0:1], head_ref[:, 1:2]
    )
    cum_t = transposed(cum)
    key = act[inner : inner + states, :].astype(BF16)
    query = act[inner + states :, :].astype(BF16)
    scores = dot_tn(key, query)
    seen = rows_of((CHUNK, CHUNK)) <= lanes_of((CHUNK, CHUNK))
    grown = jnp.exp(cum)
    last = cum[:, CHUNK - 1 :]
    to_end = jnp.exp(last - cum) * step
    fade = jnp.broadcast_to(jnp.exp(last), cum.shape)
    squares = jnp.zeros((8, CHUNK), F32)
    s_ref[0] = state[...]
    for head in range(heads):
        span = slice(head * width, (head + 1) * width)
        gap = cum[head : head + 1, :] - cum_t[:, head : head + 1]
        mixing = (scores * jnp.exp(jnp.where(seen, gap, -1e30))).astype(BF16)
        x = act[span, :]
        held = state[span, :]
        scan = dot_nn((x * step[head : head + 1, :]).astype(BF16), mixing)
        scan = scan + grown[head : head + 1, :] * dot_nn(held.astype(BF16), query)
        y_ref[span, :] = scan
        state[span, :] = fade[head : head + 1, :] * held + dot_nt(
            (x * to_end[head : head + 1, :]).astype(BF16), key
        )
        gate = z_ref[span, :].astype(F32)
        gated = (scan + row_ref[span, 1:2] * x) * (gate * sigmoid(gate))
        squares = squares + jnp.sum((gated * gated).reshape(width // 8, 8, CHUNK), axis=0)
        w_ref[span, :] = (gated * row_ref[span, 0:1]).astype(BF16)
    sq_ref[...] = squares


def forward_mix(z, conv_cols, head_cols, row_cols, dims):
    inner, heads, width, states = dims
    chans = inner + 2 * states
    rows, length = z.shape
    count = length // CHUNK
    return pl.pallas_call(
        functools.partial(forward_body, dims),
        grid=(count,),
        in_specs=[
            pl.BlockSpec((rows, CHUNK), lambda c: (0, c)),
            pl.BlockSpec(conv_cols.shape, lambda c: (0, 0)),
            pl.BlockSpec(head_cols.shape, lambda c: (0, 0)),
            pl.BlockSpec(row_cols.shape, lambda c: (0, 0)),
        ],
        out_specs=[
            pl.BlockSpec((inner, CHUNK), lambda c: (0, c)),
            pl.BlockSpec((8, CHUNK), lambda c: (0, c)),
            pl.BlockSpec((inner, CHUNK), lambda c: (0, c)),
            pl.BlockSpec((1, inner, states), lambda c: (c, 0, 0)),
        ],
        out_shape=[
            jax.ShapeDtypeStruct((inner, length), BF16),
            jax.ShapeDtypeStruct((8, length), F32),
            jax.ShapeDtypeStruct((inner, length), F32),
            jax.ShapeDtypeStruct((count, inner, states), F32),
        ],
        scratch_shapes=[
            pltpu.VMEM((chans, CHUNK), F32),
            pltpu.VMEM((chans, CHUNK), BF16),
            pltpu.VMEM((inner, states), F32),
            pltpu.VMEM((TAPS + 1, chans, CHUNK), F32),
        ],
        cost_estimate=pl.CostEstimate(
            flops=2 * length * inner * (CHUNK + 2 * states) * 2,
            bytes_accessed=rows * length * 2 + inner * length * 6 + count * inner * states * 4,
            transcendentals=length * heads * CHUNK,
        ),
        name="mix_forward",
    )(z, conv_cols, head_cols, row_cols)


def backward_body(
    dims, z_ref, zp_ref, dw_ref, r_ref, y_ref, s_ref, conv_ref, head_ref, row_ref,
    dz_ref, chan_ref, inner_ref, hsum_ref,
    act, slope, shifts, later, snext, dstate, dact, wide, acc_c, acc_i, acc_h, prod,
):
    inner, heads, width, states = dims
    chans = inner + 2 * states
    hrows = head_ref.shape[0]
    at = pl.program_id(0)
    total = pl.num_programs(0)

    @pl.when(at == 0)
    def _():
        later[...] = jnp.zeros_like(later)
        snext[...] = jnp.zeros_like(snext)
        dstate[...] = jnp.zeros_like(dstate)
        acc_c[...] = jnp.zeros_like(acc_c)
        acc_i[...] = jnp.zeros_like(acc_i)
        acc_h[...] = jnp.zeros_like(acc_h)
        for which in range(TAPS + 1):
            wide[which] = jnp.broadcast_to(conv_ref[:, which : which + 1], (chans, CHUNK))

    started = jnp.where(at == total - 1, 0.0, 1.0)
    for row in range(0, chans, width):
        span = slice(row, row + width)
        now = z_ref[inner + row : inner + row + width, :].astype(F32)
        before = zp_ref[inner + row : inner + row + width, :].astype(F32) * started
        conv = wide[TAPS, span, :] + wide[TAPS - 1, span, :] * now
        for by in range(1, TAPS):
            moved = shifted_right(now, before, by)
            shifts[by - 1, span, :] = moved
            conv = conv + wide[TAPS - 1 - by, span, :] * moved
        sig = sigmoid(conv)
        out = conv * sig
        act[span, :] = out
        slope[span, :] = sig + out * (1.0 - sig)

    raw = z_ref[inner + chans :, :].astype(F32) + head_ref[:, 0:1]
    rate = head_ref[:, 1:2]
    step, cum = decay_pieces(raw, 0.0, rate)
    cum_t = transposed(cum)
    key = act[inner : inner + states, :].astype(BF16)
    query = act[inner + states :, :].astype(BF16)
    scores = dot_tn(key, query)
    seen = rows_of((CHUNK, CHUNK)) <= lanes_of((CHUNK, CHUNK))
    grown = jnp.exp(cum)
    last = cum[:, CHUNK - 1 :]
    to_end = jnp.exp(last - cum)
    fade = jnp.broadcast_to(jnp.exp(last), cum.shape)
    dscores = jnp.zeros((CHUNK, CHUNK), F32)
    dkey = jnp.zeros((states, CHUNK), F32)
    dquery = jnp.zeros((states, CHUNK), F32)
    weight_row = r_ref[0:1, :]
    for head in range(heads):
        span = slice(head * width, (head + 1) * width)
        one = slice(head, head + 1)
        x = act[span, :]
        gate = z_ref[span, :].astype(F32)
        sg = sigmoid(gate)
        sgate = gate * sg
        scan = y_ref[span, :]
        y = scan + row_ref[span, 1:2] * x
        gated = y * sgate
        dw = dw_ref[span, :].astype(F32)
        dgated = dw * row_ref[span, 0:1] - weight_row * gated
        acc_i[0, span, :] += dw * gated
        dy = dgated * sgate
        acc_i[1, span, :] += dy * x
        dz_ref[span, :] = (dgated * y * (sg + sgate * (1.0 - sg))).astype(BF16)

        gap = cum[one, :] - cum_t[:, one]
        decay = jnp.exp(jnp.where(seen, gap, -1e30))
        mixing = (scores * decay).astype(BF16)
        dyb = dy.astype(BF16)
        xd = x * step[one, :]
        xdb = xd.astype(BF16)
        dscores = dscores + dot_tn(xdb, dyb) * decay
        dstb = dstate[span, :].astype(BF16)
        dxd = dot_nt(dyb, mixing) + to_end[one, :] * dot_nn(dstb, key)
        wxd = (xd * to_end[one, :]).astype(BF16)
        edy = (dy * grown[one, :]).astype(BF16)
        dkey = dkey + dot_tn(dstb, wxd)
        dquery = dquery + dot_tn(s_ref[0, span, :].astype(BF16), edy)
        prod[0, one, :] = jnp.sum(
            dyb.astype(F32) * scan - xdb.astype(F32) * dxd, axis=0, keepdims=True
        )
        prod[1, one, :] = jnp.sum(x * dxd, axis=0, keepdims=True)
        held = dstate[span, :]
        prod[2, one, :] = jnp.sum(snext[span, :] * held, axis=0, keepdims=True)
        dstate[span, :] = fade[one, :] * held + dot_nt(edy, query)
        dact[span, :] = step[one, :] * dxd + row_ref[span, 1:2] * dy
    snext[...] = s_ref[0]
    dsb = dscores.astype(BF16)
    dact[inner : inner + states, :] = dkey + dot_nt(query, dsb)
    dact[inner + states :, :] = dquery + dot_nn(key, dsb)

    live = rows_of((hrows, CHUNK)) < heads
    lower = (rows_of((CHUNK, CHUNK)) >= lanes_of((CHUNK, CHUNK))).astype(F32)
    zero = jnp.zeros((hrows, CHUNK), F32)
    dla = lax.dot_general(
        jnp.where(live, prod[0], zero), lower, (((1,), (0,)), ((), ())), precision=HIGH,
        preferred_element_type=F32,
    ) + jnp.sum(jnp.where(live, prod[2], zero), axis=1, keepdims=True)
    dstep = jnp.where(live, prod[1], zero) + rate * dla
    draw = dstep * sigmoid(raw)
    acc_h[0] += draw
    acc_h[1] += step * dla
    dz_ref[inner + chans :, :] = draw.astype(BF16)

    for row in range(0, chans, width):
        span = slice(row, row + width)
        dconv = dact[span, :] * slope[span, :]
        acc_c[TAPS, span, :] += dconv
        acc_c[TAPS - 1, span, :] += dconv * z_ref[inner + row : inner + row + width, :].astype(F32)
        back = wide[TAPS - 1, span, :] * dconv
        after = later[span, :]
        for by in range(1, TAPS):
            acc_c[TAPS - 1 - by, span, :] += dconv * shifts[by - 1, span, :]
            back = back + wide[TAPS - 1 - by, span, :] * shifted_left(dconv, after, by)
        later[span, :] = dconv
        dz_ref[inner + row : inner + row + width, :] = back.astype(BF16)

    @pl.when(at == total - 1)
    def _():
        ones = jnp.ones((8, CHUNK), F32)

        def sums(block):
            return lax.dot_general(
                ones, block, (((1,), (1,)), ((), ())), precision=HIGH, preferred_element_type=F32
            )

        for which in range(TAPS + 1):
            chan_ref[which] = sums(acc_c[which])
        for which in range(2):
            inner_ref[which] = sums(acc_i[which])
            hsum_ref[which] = acc_h[which]


def backward_mix(z, dw, r, y, s, conv_cols, head_cols, row_cols, dims):
    inner, heads, width, states = dims
    chans = inner + 2 * states
    rows, length = z.shape
    hrows = head_cols.shape[0]
    count = length // CHUNK
    back = lambda c: (0, count - 1 - c)
    return pl.pallas_call(
        functools.partial(backward_body, dims),
        grid=(count,),
        in_specs=[
            pl.BlockSpec((rows, CHUNK), back),
            pl.BlockSpec((rows, CHUNK), lambda c: (0, jnp.maximum(count - 2 - c, 0))),
            pl.BlockSpec((inner, CHUNK), back),
            pl.BlockSpec((8, CHUNK), back),
            pl.BlockSpec((inner, CHUNK), back),
            pl.BlockSpec((1, inner, states), lambda c: (count - 1 - c, 0, 0)),
            pl.BlockSpec(conv_cols.shape, lambda c: (0, 0)),
            pl.BlockSpec(head_cols.shape, lambda c: (0, 0)),
            pl.BlockSpec(row_cols.shape, lambda c: (0, 0)),
        ],
        out_specs=[
            pl.BlockSpec((rows, CHUNK), back),
            pl.BlockSpec((TAPS + 1, 8, chans), lambda c: (0, 0, 0)),
            pl.BlockSpec((2, 8, inner), lambda c: (0, 0, 0)),
            pl.BlockSpec((2, hrows, CHUNK), lambda c: (0, 0, 0)),
        ],
        out_shape=[
            jax.ShapeDtypeStruct((rows, length), BF16),
            jax.ShapeDtypeStruct((TAPS + 1, 8, chans), F32),
            jax.ShapeDtypeStruct((2, 8, inner), F32),
            jax.ShapeDtypeStruct((2, hrows, CHUNK), F32),
        ],
        scratch_shapes=[
            pltpu.VMEM((chans, CHUNK), F32),
            pltpu.VMEM((chans, CHUNK), F32),
            pltpu.VMEM((TAPS - 1, chans, CHUNK), F32),
            pltpu.VMEM((chans, CHUNK), F32),
            pltpu.VMEM((inner, states), F32),
            pltpu.VMEM((inner, states), F32),
            pltpu.VMEM((chans, CHUNK), F32),
            pltpu.VMEM((TAPS + 1, chans, CHUNK), F32),
            pltpu.VMEM((TAPS + 1, chans, CHUNK), F32),
            pltpu.VMEM((2, inner, CHUNK), F32),
            pltpu.VMEM((2, hrows, CHUNK), F32),
            pltpu.VMEM((3, hrows, CHUNK), F32),
        ],
        cost_estimate=pl.CostEstimate(
            flops=4 * length * inner * (CHUNK + 2 * states) * 2,
            bytes_accessed=rows * length * 6 + inner * length * 6 + count * inner * states * 4,
            transcendentals=length * heads * CHUNK,
        ),
        name="mix_backward",
    )(z, z, dw, r, y, s, conv_cols, head_cols, row_cols)


SMALLS = 9


def per_device(
    block_input,
    zx_weight,
    bc_weight,
    dt_weight,
    out_weight,
    norm_gain,
    inner_conv,
    inner_conv_bias,
    state_conv,
    state_conv_bias,
    dt_bias,
    a_log,
    d_skip,
    gated_gain,
    cotangent,
):
    layers, _, shard, inner = zx_weight.shape
    sequences, length, model = block_input.shape
    pair = bc_weight.shape[2]
    states = pair // 2
    heads = dt_weight.shape[2]
    width = inner // heads
    inner_total = inner * lax.axis_size("mp")
    hrows = -(-heads // 16) * 16
    chans = inner + pair
    dims = (inner, heads, width, states)

    in_full, out_full, cols = [], [], []
    for layer in range(layers):
        packed = jnp.concatenate(
            [
                zx_weight[layer, 0],
                zx_weight[layer, 1],
                bc_weight[layer],
                jnp.pad(dt_weight[layer], ((0, 0), (0, hrows - heads))),
            ],
            axis=1,
        )
        in_full.append(lax.all_gather(packed, "dp", axis=0, tiled=True))
        out_full.append(lax.all_gather(out_weight[layer].T, "dp", axis=0, tiled=True))
        taps = jnp.concatenate([inner_conv[layer], state_conv[layer]], axis=1)
        offset = jnp.concatenate([inner_conv_bias[layer], state_conv_bias[layer]])
        conv_cols = jnp.pad(jnp.concatenate([taps, offset[None]], axis=0), ((0, 3), (0, 0))).T
        head_cols = jnp.pad(
            jnp.stack([dt_bias[layer], -jnp.exp(a_log[layer])], axis=1),
            ((0, hrows - heads), (0, 6)),
        )
        row_cols = jnp.pad(
            jnp.stack([gated_gain[layer], jnp.repeat(d_skip[layer], width)], axis=1),
            ((0, 0), (0, 6)),
        )
        cols.append((conv_cols, head_cols, row_cols))

    def forward_layer(layer, hidden):
        root = lax.rsqrt(jnp.mean(hidden * hidden, axis=-1) + EPS)
        normed = (hidden * root[:, None] * norm_gain[layer][None, :]).astype(BF16)
        z = jnp.einsum("df,td->ft", in_full[layer], normed, preferred_element_type=F32).astype(BF16)
        weighted, squares, scan, held = forward_mix(z, *cols[layer], dims)
        partial = jnp.einsum(
            "it,di->td", weighted, out_full[layer], preferred_element_type=F32
        ).astype(BF16)
        summed = lax.psum(partial, "mp").astype(F32)
        scale = lax.rsqrt(lax.psum(jnp.sum(squares, axis=0), "mp") / inner_total + EPS)
        kept = (hidden, root, normed, z, weighted, scan, held, scale, summed)
        return hidden + scale[:, None] * summed, kept

    def backward_layer(layer, kept, grad):
        hidden, root, normed, z, weighted, scan, held, scale, summed = kept
        dsummed = (scale[:, None] * grad).astype(BF16)
        dscale = jnp.sum(grad * summed, axis=-1)
        ratio = dscale * scale**3 / inner_total
        dweighted = jnp.einsum(
            "td,di->it", dsummed, out_full[layer], preferred_element_type=F32
        ).astype(BF16)
        dz, dchan, dinner, dheads = backward_mix(
            z, dweighted, jnp.broadcast_to(ratio, (8, length)), scan, held, *cols[layer], dims
        )
        partial = jnp.einsum("ft,df->td", dz, in_full[layer], preferred_element_type=F32).astype(
            BF16
        )
        dnormed = lax.psum(partial, "mp").astype(F32)
        unit = hidden * root[:, None]
        dnorm = jnp.sum(dnormed * unit, axis=0)
        back = dnormed * norm_gain[layer][None, :]
        grad = grad + root[:, None] * (
            back - unit * jnp.mean(back * unit, axis=-1, keepdims=True)
        )
        return grad, (normed, dz, dsummed, weighted), (dnorm, dchan, dinner, dheads)

    hidden = [block_input[seq].astype(F32) for seq in range(sequences)]
    kept = [[None] * sequences for _ in range(layers)]
    for layer in range(layers):
        for seq in range(sequences):
            hidden[seq], kept[layer][seq] = forward_layer(layer, hidden[seq])
    outputs = jnp.stack([item.astype(BF16) for item in hidden])

    grad = [cotangent[seq].astype(F32) for seq in range(sequences)]
    in_grads, out_grads, small_grads = [None] * layers, [None] * layers, [None] * layers
    for layer in reversed(range(layers)):
        bigs, smalls = [], []
        for seq in range(sequences):
            grad[seq], big, small = backward_layer(layer, kept[layer][seq], grad[seq])
            bigs.append(big)
            smalls.append(small)
        out_term = sum(
            jnp.einsum("td,it->di", big[2], big[3], preferred_element_type=F32) for big in bigs
        )
        in_term = sum(
            jnp.einsum("td,ft->df", big[0], big[1], preferred_element_type=F32) for big in bigs
        )
        out_grads[layer] = lax.psum_scatter(
            out_term.astype(BF16), "dp", scatter_dimension=0, tiled=True
        )
        in_grads[layer] = lax.psum_scatter(
            in_term.astype(BF16), "dp", scatter_dimension=0, tiled=True
        )
        small_grads[layer] = [sum(parts) for parts in zip(*smalls)]
    input_grad = jnp.stack(grad)

    out_grad = jnp.stack([item.T for item in out_grads]).astype(F32)
    in_grad = jnp.stack(in_grads)
    zx_grad = jnp.stack([in_grad[:, :, :inner], in_grad[:, :, inner : 2 * inner]], axis=1)
    zx_grad = zx_grad.astype(F32)
    dt_grad = in_grad[:, :, 2 * inner + pair : 2 * inner + pair + heads].astype(F32)
    bc_part = in_grad[:, :, 2 * inner : 2 * inner + pair]

    dnorm = jnp.stack([item[0] for item in small_grads])
    dchan = jnp.stack([item[1][:, 0] for item in small_grads])
    dinner = jnp.stack([item[2][:, 0] for item in small_grads])
    dheads = jnp.stack([jnp.sum(item[3], axis=-1)[:, :heads] for item in small_grads])
    dskip = jnp.sum(dinner[:, 1].reshape(layers, heads, width), axis=-1)
    dlog = dheads[:, 1] * -jnp.exp(a_log)
    vector = jnp.concatenate(
        [dnorm, dchan.reshape(layers, -1), dinner[:, 0], dheads[:, 0], dlog, dskip], axis=1
    )
    vector = lax.psum(vector, "dp")
    spots = [model, model + (TAPS + 1) * chans]
    spots += [spots[1] + inner]
    spots += [spots[2] + heads, spots[2] + 2 * heads]
    dnorm, dchan, dgain, dbias, dlog, dskip = jnp.split(vector, spots, axis=1)
    dchan = dchan.reshape(layers, TAPS + 1, chans)
    shared = lax.psum(
        jnp.concatenate(
            [bc_part.reshape(-1).astype(F32), dchan[:, :, inner:].reshape(-1)]
        ).astype(BF16),
        "mp",
    ).astype(F32)
    cut = bc_part.size
    bc_grad = shared[:cut].reshape(bc_part.shape)
    dstate = shared[cut:].reshape(layers, TAPS + 1, pair)
    return (
        outputs,
        input_grad,
        zx_grad,
        bc_grad,
        dt_grad,
        out_grad,
        dnorm,
        dchan[:, :TAPS, :inner],
        dchan[:, TAPS, :inner],
        dstate[:, :TAPS],
        dstate[:, TAPS],
        dbias,
        dlog,
        dskip,
        dgain,
    )


def solution(mesh):
    placed = (
        P("dp", None, None),
        P(None, None, "dp", "mp"),
        P(None, "dp", None),
        P(None, "dp", "mp"),
        P(None, "mp", "dp"),
        P(),
        P(None, None, "mp"),
        P(None, "mp"),
        P(),
        P(),
        P(None, "mp"),
        P(None, "mp"),
        P(None, "mp"),
        P(None, "mp"),
        P("dp", None, None),
    )
    return jax.shard_map(
        per_device,
        mesh=mesh,
        in_specs=placed,
        out_specs=(
            P("dp", None, None),
            P("dp", None, None),
            P(None, None, "dp", "mp"),
            P(None, "dp", None),
            P(None, "dp", "mp"),
            P(None, "mp", "dp"),
            P(),
            P(None, None, "mp"),
            P(None, "mp"),
            P(),
            P(),
            P(None, "mp"),
            P(None, "mp"),
            P(None, "mp"),
            P(None, "mp"),
        ),
        check_vma=False,
    )
```

```python
import functools

import jax
import jax.numpy as jnp
from jax import lax
from jax.experimental import pallas as pl
from jax.experimental.pallas import tpu as pltpu
from jax.sharding import PartitionSpec as P

EPS = 1e-05
HIGH = lax.Precision.HIGHEST
CHUNK = 128
TAPS = 4
F32 = jnp.float32
BF16 = jnp.bfloat16


def dot_nn(a, b):
    return lax.dot_general(a, b, (((1,), (0,)), ((), ())), preferred_element_type=F32)


def dot_nt(a, b):
    return lax.dot_general(a, b, (((1,), (1,)), ((), ())), preferred_element_type=F32)


def dot_tn(a, b):
    return lax.dot_general(a, b, (((0,), (0,)), ((), ())), preferred_element_type=F32)


def sigmoid(v):
    return 0.5 * jnp.tanh(0.5 * v) + 0.5


def softplus(v):
    return jnp.maximum(v, 0.0) + jnp.log1p(jnp.exp(-jnp.abs(v)))


def lanes_of(shape):
    return lax.broadcasted_iota(jnp.int32, shape, 1)


def rows_of(shape):
    return lax.broadcasted_iota(jnp.int32, shape, 0)


def shifted_right(now, before, by):
    merged = jnp.where(lanes_of(now.shape) >= CHUNK - by, before, now)
    return pltpu.roll(merged, by, 1)


def shifted_left(now, after, by):
    merged = jnp.where(lanes_of(now.shape) < by, after, now)
    return pltpu.roll(merged, CHUNK - by, 1)


def decay_pieces(raw, bias, rate):
    step = softplus(raw + bias)
    upper = (rows_of((CHUNK, CHUNK)) <= lanes_of((CHUNK, CHUNK))).astype(F32)
    cum = lax.dot_general(
        step * rate, upper, (((1,), (0,)), ((), ())), precision=HIGH, preferred_element_type=F32
    )
    return step, cum


def transposed(a):
    rows = a.shape[0]
    padded = jnp.concatenate([a, jnp.zeros((CHUNK - rows, CHUNK), F32)], axis=0)
    return jnp.transpose(padded)


def forward_body(dims, flip_ref, z_ref, conv_ref, head_ref, row_ref, w_ref, sq_ref, y_ref, s_ref, act, tail, state, wide):
    inner, heads, width, states = dims
    chans = inner + 2 * states
    at = pl.program_id(0)

    @pl.when(at == 0)
    def _():
        tail[...] = jnp.zeros_like(tail)
        state[...] = jnp.zeros_like(state)
        for which in range(TAPS + 1):
            wide[which] = jnp.broadcast_to(conv_ref[:, which : which + 1], (chans, CHUNK))

    for row in range(0, chans, width):
        span = slice(row, row + width)
        now = z_ref[inner + row : inner + row + width, :].astype(F32)
        before = tail[span, :].astype(F32)
        conv = wide[TAPS, span, :] + wide[TAPS - 1, span, :] * now
        for by in range(1, TAPS):
            conv = conv + wide[TAPS - 1 - by, span, :] * shifted_right(now, before, by)
        act[span, :] = conv * sigmoid(conv)
    tail[...] = z_ref[inner : inner + chans, :]

    step, cum = decay_pieces(
        z_ref[inner + chans :, :].astype(F32), head_ref[:, 0:1], head_ref[:, 1:2]
    )
    cum_t = transposed(cum)
    key = act[inner : inner + states, :].astype(BF16)
    query = act[inner + states :, :].astype(BF16)
    scores = dot_tn(key, query)
    seen = rows_of((CHUNK, CHUNK)) <= lanes_of((CHUNK, CHUNK))
    grown = jnp.exp(cum)
    last = cum[:, CHUNK - 1 :]
    to_end = jnp.exp(last - cum) * step
    fade = jnp.broadcast_to(jnp.exp(last), cum.shape)
    squares = jnp.zeros((8, CHUNK), F32)
    s_ref[0] = state[...]
    for head in range(heads):
        span = slice(head * width, (head + 1) * width)
        gap = cum[head : head + 1, :] - cum_t[:, head : head + 1]
        mixing = (scores * jnp.exp(jnp.where(seen, gap, -1e30))).astype(BF16)
        x = act[span, :]
        held = state[span, :]
        scan = dot_nn((x * step[head : head + 1, :]).astype(BF16), mixing)
        scan = scan + grown[head : head + 1, :] * dot_nn(held.astype(BF16), query)
        y_ref[span, :] = scan
        state[span, :] = fade[head : head + 1, :] * held + dot_nt(
            (x * to_end[head : head + 1, :]).astype(BF16), key
        )
        gate = z_ref[span, :].astype(F32)
        gated = (scan + row_ref[span, 1:2] * x) * (gate * sigmoid(gate))
        squares = squares + jnp.sum((gated * gated).reshape(width // 8, 8, CHUNK), axis=0)
        w_ref[span, :] = (gated * row_ref[span, 0:1]).astype(BF16)
    sq_ref[...] = squares


def time_block(step, count, flip_ref):
    return lax.rem(step + flip_ref[0] * (count // 2), count)


def forward_mix(flip, z, conv_cols, head_cols, row_cols, dims):
    inner, heads, width, states = dims
    chans = inner + 2 * states
    rows, length = z.shape
    count = length // CHUNK
    here = lambda c, flip_ref: (0, time_block(c, count, flip_ref))
    whole = lambda c, flip_ref: (0, 0)
    return pl.pallas_call(
        functools.partial(forward_body, dims),
        grid_spec=pltpu.PrefetchScalarGridSpec(
            num_scalar_prefetch=1,
            grid=(count,),
            in_specs=[
                pl.BlockSpec((rows, CHUNK), here),
                pl.BlockSpec(conv_cols.shape, whole),
                pl.BlockSpec(head_cols.shape, whole),
                pl.BlockSpec(row_cols.shape, whole),
            ],
            out_specs=[
                pl.BlockSpec((inner, CHUNK), here),
                pl.BlockSpec((8, CHUNK), here),
                pl.BlockSpec((inner, CHUNK), here),
                pl.BlockSpec((1, inner, states), lambda c, flip_ref: (c, 0, 0)),
            ],
            scratch_shapes=[
                pltpu.VMEM((chans, CHUNK), F32),
                pltpu.VMEM((chans, CHUNK), BF16),
                pltpu.VMEM((inner, states), F32),
                pltpu.VMEM((TAPS + 1, chans, CHUNK), F32),
            ],
        ),
        out_shape=[
            jax.ShapeDtypeStruct((inner, length), BF16),
            jax.ShapeDtypeStruct((8, length), F32),
            jax.ShapeDtypeStruct((inner, length), F32),
            jax.ShapeDtypeStruct((count, inner, states), F32),
        ],
        cost_estimate=pl.CostEstimate(
            flops=2 * length * inner * (CHUNK + 2 * states) * 2,
            bytes_accessed=rows * length * 2 + inner * length * 6 + count * inner * states * 4,
            transcendentals=length * heads * CHUNK,
        ),
        name="mix_forward",
    )(flip, z, conv_cols, head_cols, row_cols)


def backward_body(
    dims, flip_ref, z_ref, zp_ref, dw_ref, r_ref, y_ref, s_ref, conv_ref, head_ref, row_ref,
    dz_ref, chan_ref, inner_ref, hsum_ref,
    act, slope, shifts, later, snext, dstate, dact, wide, acc_c, acc_i, acc_h, prod,
):
    inner, heads, width, states = dims
    chans = inner + 2 * states
    hrows = head_ref.shape[0]
    at = pl.program_id(0)
    total = pl.num_programs(0)

    @pl.when(at == 0)
    def _():
        later[...] = jnp.zeros_like(later)
        snext[...] = jnp.zeros_like(snext)
        dstate[...] = jnp.zeros_like(dstate)
        acc_c[...] = jnp.zeros_like(acc_c)
        acc_i[...] = jnp.zeros_like(acc_i)
        acc_h[...] = jnp.zeros_like(acc_h)
        for which in range(TAPS + 1):
            wide[which] = jnp.broadcast_to(conv_ref[:, which : which + 1], (chans, CHUNK))

    started = jnp.where(at == total - 1, 0.0, 1.0)
    for row in range(0, chans, width):
        span = slice(row, row + width)
        now = z_ref[inner + row : inner + row + width, :].astype(F32)
        before = zp_ref[inner + row : inner + row + width, :].astype(F32) * started
        conv = wide[TAPS, span, :] + wide[TAPS - 1, span, :] * now
        for by in range(1, TAPS):
            moved = shifted_right(now, before, by)
            shifts[by - 1, span, :] = moved
            conv = conv + wide[TAPS - 1 - by, span, :] * moved
        sig = sigmoid(conv)
        out = conv * sig
        act[span, :] = out
        slope[span, :] = sig + out * (1.0 - sig)

    raw = z_ref[inner + chans :, :].astype(F32) + head_ref[:, 0:1]
    rate = head_ref[:, 1:2]
    step, cum = decay_pieces(raw, 0.0, rate)
    cum_t = transposed(cum)
    key = act[inner : inner + states, :].astype(BF16)
    query = act[inner + states :, :].astype(BF16)
    scores = dot_tn(key, query)
    seen = rows_of((CHUNK, CHUNK)) <= lanes_of((CHUNK, CHUNK))
    grown = jnp.exp(cum)
    last = cum[:, CHUNK - 1 :]
    to_end = jnp.exp(last - cum)
    fade = jnp.broadcast_to(jnp.exp(last), cum.shape)
    dscores = jnp.zeros((CHUNK, CHUNK), F32)
    dkey = jnp.zeros((states, CHUNK), F32)
    dquery = jnp.zeros((states, CHUNK), F32)
    weight_row = r_ref[0:1, :]
    for head in range(heads):
        span = slice(head * width, (head + 1) * width)
        one = slice(head, head + 1)
        x = act[span, :]
        gate = z_ref[span, :].astype(F32)
        sg = sigmoid(gate)
        sgate = gate * sg
        scan = y_ref[span, :]
        y = scan + row_ref[span, 1:2] * x
        gated = y * sgate
        dw = dw_ref[span, :].astype(F32)
        dgated = dw * row_ref[span, 0:1] - weight_row * gated
        acc_i[0, span, :] += dw * gated
        dy = dgated * sgate
        acc_i[1, span, :] += dy * x
        dz_ref[span, :] = (dgated * y * (sg + sgate * (1.0 - sg))).astype(BF16)

        gap = cum[one, :] - cum_t[:, one]
        decay = jnp.exp(jnp.where(seen, gap, -1e30))
        mixing = (scores * decay).astype(BF16)
        dyb = dy.astype(BF16)
        xd = x * step[one, :]
        xdb = xd.astype(BF16)
        dscores = dscores + dot_tn(xdb, dyb) * decay
        dstb = dstate[span, :].astype(BF16)
        dxd = dot_nt(dyb, mixing) + to_end[one, :] * dot_nn(dstb, key)
        wxd = (xd * to_end[one, :]).astype(BF16)
        edy = (dy * grown[one, :]).astype(BF16)
        dkey = dkey + dot_tn(dstb, wxd)
        dquery = dquery + dot_tn(s_ref[0, span, :].astype(BF16), edy)
        prod[0, one, :] = jnp.sum(
            dyb.astype(F32) * scan - xdb.astype(F32) * dxd, axis=0, keepdims=True
        )
        prod[1, one, :] = jnp.sum(x * dxd, axis=0, keepdims=True)
        held = dstate[span, :]
        prod[2, one, :] = jnp.sum(snext[span, :] * held, axis=0, keepdims=True)
        dstate[span, :] = fade[one, :] * held + dot_nt(edy, query)
        dact[span, :] = step[one, :] * dxd + row_ref[span, 1:2] * dy
    snext[...] = s_ref[0]
    dsb = dscores.astype(BF16)
    dact[inner : inner + states, :] = dkey + dot_nt(query, dsb)
    dact[inner + states :, :] = dquery + dot_nn(key, dsb)

    live = rows_of((hrows, CHUNK)) < heads
    lower = (rows_of((CHUNK, CHUNK)) >= lanes_of((CHUNK, CHUNK))).astype(F32)
    zero = jnp.zeros((hrows, CHUNK), F32)
    dla = lax.dot_general(
        jnp.where(live, prod[0], zero), lower, (((1,), (0,)), ((), ())), precision=HIGH,
        preferred_element_type=F32,
    ) + jnp.sum(jnp.where(live, prod[2], zero), axis=1, keepdims=True)
    dstep = jnp.where(live, prod[1], zero) + rate * dla
    draw = dstep * sigmoid(raw)
    acc_h[0] += draw
    acc_h[1] += step * dla
    dz_ref[inner + chans :, :] = draw.astype(BF16)

    for row in range(0, chans, width):
        span = slice(row, row + width)
        dconv = dact[span, :] * slope[span, :]
        acc_c[TAPS, span, :] += dconv
        acc_c[TAPS - 1, span, :] += dconv * z_ref[inner + row : inner + row + width, :].astype(F32)
        back = wide[TAPS - 1, span, :] * dconv
        after = later[span, :]
        for by in range(1, TAPS):
            acc_c[TAPS - 1 - by, span, :] += dconv * shifts[by - 1, span, :]
            back = back + wide[TAPS - 1 - by, span, :] * shifted_left(dconv, after, by)
        later[span, :] = dconv
        dz_ref[inner + row : inner + row + width, :] = back.astype(BF16)

    @pl.when(at == total - 1)
    def _():
        ones = jnp.ones((8, CHUNK), F32)

        def sums(block):
            return lax.dot_general(
                ones, block, (((1,), (1,)), ((), ())), precision=HIGH, preferred_element_type=F32
            )

        for which in range(TAPS + 1):
            chan_ref[which] = sums(acc_c[which])
        for which in range(2):
            inner_ref[which] = sums(acc_i[which])
            hsum_ref[which] = acc_h[which]


def backward_mix(flip, z, dw, r, y, s, conv_cols, head_cols, row_cols, dims):
    inner, heads, width, states = dims
    chans = inner + 2 * states
    rows, length = z.shape
    hrows = head_cols.shape[0]
    count = length // CHUNK
    back = lambda c, flip_ref: (0, time_block(count - 1 - c, count, flip_ref))
    whole = lambda c, flip_ref: (0, 0)
    whole3 = lambda c, flip_ref: (0, 0, 0)
    return pl.pallas_call(
        functools.partial(backward_body, dims),
        grid_spec=pltpu.PrefetchScalarGridSpec(
            num_scalar_prefetch=1,
            grid=(count,),
            in_specs=[
                pl.BlockSpec((rows, CHUNK), back),
                pl.BlockSpec(
                    (rows, CHUNK),
                    lambda c, flip_ref: (
                        0,
                        time_block(jnp.maximum(count - 2 - c, 0), count, flip_ref),
                    ),
                ),
                pl.BlockSpec((inner, CHUNK), back),
                pl.BlockSpec((8, CHUNK), back),
                pl.BlockSpec((inner, CHUNK), back),
                pl.BlockSpec((1, inner, states), lambda c, flip_ref: (count - 1 - c, 0, 0)),
                pl.BlockSpec(conv_cols.shape, whole),
                pl.BlockSpec(head_cols.shape, whole),
                pl.BlockSpec(row_cols.shape, whole),
            ],
            out_specs=[
                pl.BlockSpec((rows, CHUNK), back),
                pl.BlockSpec((TAPS + 1, 8, chans), whole3),
                pl.BlockSpec((2, 8, inner), whole3),
                pl.BlockSpec((2, hrows, CHUNK), whole3),
            ],
            scratch_shapes=[
                pltpu.VMEM((chans, CHUNK), F32),
                pltpu.VMEM((chans, CHUNK), F32),
                pltpu.VMEM((TAPS - 1, chans, CHUNK), F32),
                pltpu.VMEM((chans, CHUNK), F32),
                pltpu.VMEM((inner, states), F32),
                pltpu.VMEM((inner, states), F32),
                pltpu.VMEM((chans, CHUNK), F32),
                pltpu.VMEM((TAPS + 1, chans, CHUNK), F32),
                pltpu.VMEM((TAPS + 1, chans, CHUNK), F32),
                pltpu.VMEM((2, inner, CHUNK), F32),
                pltpu.VMEM((2, hrows, CHUNK), F32),
                pltpu.VMEM((3, hrows, CHUNK), F32),
            ],
        ),
        out_shape=[
            jax.ShapeDtypeStruct((rows, length), BF16),
            jax.ShapeDtypeStruct((TAPS + 1, 8, chans), F32),
            jax.ShapeDtypeStruct((2, 8, inner), F32),
            jax.ShapeDtypeStruct((2, hrows, CHUNK), F32),
        ],
        cost_estimate=pl.CostEstimate(
            flops=4 * length * inner * (CHUNK + 2 * states) * 2,
            bytes_accessed=rows * length * 6 + inner * length * 6 + count * inner * states * 4,
            transcendentals=length * heads * CHUNK,
        ),
        name="mix_backward",
    )(flip, z, z, dw, r, y, s, conv_cols, head_cols, row_cols)


def per_device(
    block_input,
    zx_weight,
    bc_weight,
    dt_weight,
    out_weight,
    norm_gain,
    inner_conv,
    inner_conv_bias,
    state_conv,
    state_conv_bias,
    dt_bias,
    a_log,
    d_skip,
    gated_gain,
    cotangent,
):
    layers, _, shard, inner = zx_weight.shape
    sequences, length, model = block_input.shape
    pair = bc_weight.shape[2]
    states = pair // 2
    heads = dt_weight.shape[2]
    width = inner // heads
    inner_total = inner * lax.axis_size("mp")
    hrows = -(-heads // 16) * 16
    chans = inner + pair
    dims = (inner, heads, width, states)

    in_full, out_full, cols = [], [], []
    for layer in range(layers):
        packed = jnp.concatenate(
            [
                zx_weight[layer, 0],
                zx_weight[layer, 1],
                bc_weight[layer],
                jnp.pad(dt_weight[layer], ((0, 0), (0, hrows - heads))),
            ],
            axis=1,
        )
        in_full.append(lax.all_gather(packed, "dp", axis=0, tiled=True))
        out_full.append(lax.all_gather(out_weight[layer].T, "dp", axis=0, tiled=True))
        taps = jnp.concatenate([inner_conv[layer], state_conv[layer]], axis=1)
        offset = jnp.concatenate([inner_conv_bias[layer], state_conv_bias[layer]])
        conv_cols = jnp.pad(jnp.concatenate([taps, offset[None]], axis=0), ((0, 3), (0, 0))).T
        head_cols = jnp.pad(
            jnp.stack([dt_bias[layer], -jnp.exp(a_log[layer])], axis=1),
            ((0, hrows - heads), (0, 6)),
        )
        row_cols = jnp.pad(
            jnp.stack([gated_gain[layer], jnp.repeat(d_skip[layer], width)], axis=1),
            ((0, 0), (0, 6)),
        )
        cols.append((conv_cols, head_cols, row_cols))

    group = lax.axis_size("mp")
    ranks = lax.axis_size("dp")
    rank = lax.axis_index("mp")
    core = lax.rem(rank, 2)
    half = length // 2
    flip = core.astype(jnp.int32).reshape(1)

    def swap(value, bit, axis="mp"):
        size = group if axis == "mp" else ranks
        return lax.ppermute(value, axis, [(at, at ^ bit) for at in range(size)])

    def own_first(value):
        mine = lax.dynamic_slice_in_dim(value, core * half, half)
        other = lax.dynamic_slice_in_dim(value, (1 - core) * half, half)
        return jnp.concatenate([mine, other], axis=0)

    def in_order(mine):
        other = swap(mine, 1)
        return jnp.where(
            core == 0,
            jnp.concatenate([mine, other], axis=0),
            jnp.concatenate([other, mine], axis=0),
        )

    def joined(mine):
        return jnp.concatenate([mine, swap(mine, 1)], axis=0)

    def sum_own(theirs, mine):
        got = swap(theirs, 1)
        total = mine.astype(F32) + got.astype(F32)
        bit = 2
        while bit < group:
            sent = total.astype(BF16)
            total = sent.astype(F32) + swap(sent, bit).astype(F32)
            bit *= 2
        return total

    def sum_rows(values):
        total = values[:half]
        for bits in range(1, group):
            total = total + swap(values[half:] if bits % 2 else values[:half], bits)
        return total

    def sum_all(value, axis):
        bit = 1
        while bit < (group if axis == "mp" else ranks):
            value = value + swap(value, bit, axis)
            bit *= 2
        return value

    def normalized(layer, hidden):
        root = lax.rsqrt(jnp.mean(hidden * hidden, axis=-1) + EPS)
        return root, (hidden * root[:, None] * norm_gain[layer][None, :]).astype(BF16)

    def forward_layer(layer, hidden, root, normed):
        z = jnp.einsum("df,td->ft", in_full[layer], normed, preferred_element_type=F32).astype(BF16)
        weighted, squares, scan, held = forward_mix(flip, z, *cols[layer], dims)
        theirs, mine = (
            jnp.einsum("it,di->td", part, out_full[layer], preferred_element_type=F32).astype(BF16)
            for part in (weighted[:, half:], weighted[:, :half])
        )
        scale = lax.rsqrt(sum_rows(jnp.sum(squares, axis=0)) / inner_total + EPS)
        summed = sum_own(theirs, mine)
        kept = (hidden, root, normed, z, weighted, scan, held, scale, summed)
        return hidden + scale[:, None] * summed, kept

    def backward_layer(layer, kept, grad):
        hidden, root, normed, z, weighted, scan, held, scale, summed = kept
        dsummed = joined((scale[:, None] * grad).astype(BF16))
        dscale = jnp.sum(grad * summed, axis=-1)
        ratio = joined(dscale * scale**3 / inner_total)
        dweighted = jnp.einsum(
            "td,di->it", dsummed, out_full[layer], preferred_element_type=F32
        ).astype(BF16)
        dz, dchan, dinner, dheads = backward_mix(
            flip, z, dweighted, jnp.broadcast_to(ratio, (8, length)), scan, held, *cols[layer], dims
        )
        theirs, mine = (
            jnp.einsum("ft,df->td", part, in_full[layer], preferred_element_type=F32).astype(BF16)
            for part in (dz[:, half:], dz[:, :half])
        )
        dnormed = sum_own(theirs, mine)
        unit = hidden * root[:, None]
        dnorm = jnp.sum(dnormed * unit, axis=0)
        back = dnormed * norm_gain[layer][None, :]
        grad = grad + root[:, None] * (
            back - unit * jnp.mean(back * unit, axis=-1, keepdims=True)
        )
        return grad, (normed, dz, dsummed, weighted), (dnorm, dchan, dinner, dheads)

    hidden = [
        lax.dynamic_slice_in_dim(block_input[seq], core * half, half).astype(F32)
        for seq in range(sequences)
    ]
    kept = [[None] * sequences for _ in range(layers)]
    for layer in range(layers):
        for seq in range(sequences):
            root, normed = normalized(layer, hidden[seq])
            if layer == 0:
                normed = normalized(layer, own_first(block_input[seq]).astype(F32))[1]
            else:
                normed = joined(normed)
            hidden[seq], kept[layer][seq] = forward_layer(layer, hidden[seq], root, normed)
    outputs = jnp.stack([in_order(item.astype(BF16)) for item in hidden])

    grad = [
        lax.dynamic_slice_in_dim(cotangent[seq], core * half, half).astype(F32)
        for seq in range(sequences)
    ]
    in_grads, out_grads, small_grads = [None] * layers, [None] * layers, [None] * layers
    for layer in reversed(range(layers)):
        bigs, smalls = [], []
        for seq in range(sequences):
            grad[seq], big, small = backward_layer(layer, kept[layer][seq], grad[seq])
            bigs.append(big)
            smalls.append(small)
        out_term = sum(
            jnp.einsum("td,it->di", big[2], big[3], preferred_element_type=F32) for big in bigs
        )
        in_term = sum(
            jnp.einsum("td,ft->df", big[0], big[1], preferred_element_type=F32) for big in bigs
        )
        out_grads[layer] = lax.psum_scatter(
            out_term.astype(BF16), "dp", scatter_dimension=0, tiled=True
        )
        in_grads[layer] = lax.psum_scatter(
            in_term.astype(BF16), "dp", scatter_dimension=0, tiled=True
        )
        small_grads[layer] = [sum(parts) for parts in zip(*smalls)]
    input_grad = jnp.stack([in_order(item.astype(BF16)).astype(F32) for item in grad])

    out_grad = jnp.stack([item.T for item in out_grads]).astype(F32)
    in_grad = jnp.stack(in_grads)
    zx_grad = jnp.stack([in_grad[:, :, :inner], in_grad[:, :, inner : 2 * inner]], axis=1)
    zx_grad = zx_grad.astype(F32)
    dt_grad = in_grad[:, :, 2 * inner + pair : 2 * inner + pair + heads].astype(F32)
    bc_part = in_grad[:, :, 2 * inner : 2 * inner + pair]

    bc_grad = sum_all(bc_part.astype(F32), "mp")
    dnorm = jnp.stack([item[0] for item in small_grads])
    dchan = jnp.stack([item[1][:, 0] for item in small_grads])
    dinner = jnp.stack([item[2][:, 0] for item in small_grads])
    dheads = jnp.stack([jnp.sum(item[3], axis=-1)[:, :heads] for item in small_grads])
    dskip = jnp.sum(dinner[:, 1].reshape(layers, heads, width), axis=-1)
    dlog = dheads[:, 1] * -jnp.exp(a_log)
    parts = [
        dnorm,
        dchan[:, :, inner:].reshape(layers, -1),
        dchan[:, :, :inner].reshape(layers, -1),
        dinner[:, 0],
        dheads[:, 0],
        dlog,
        dskip,
    ]
    spots, at = [], 0
    for part in parts[:-1]:
        at += part.shape[1]
        spots.append(at)
    vector = sum_all(jnp.concatenate(parts, axis=1), "dp")
    shared = sum_all(vector[:, : spots[1]], "mp")
    dnorm = shared[:, : spots[0]] * (2.0 / group)
    dstate = shared[:, spots[0] :].reshape(layers, TAPS + 1, pair)
    _, _, dlocal, dgain, dbias, dlog, dskip = jnp.split(vector, spots, axis=1)
    dlocal = dlocal.reshape(layers, TAPS + 1, inner)
    return (
        outputs,
        input_grad,
        zx_grad,
        bc_grad,
        dt_grad,
        out_grad,
        dnorm,
        dlocal[:, :TAPS],
        dlocal[:, TAPS],
        dstate[:, :TAPS],
        dstate[:, TAPS],
        dbias,
        dlog,
        dskip,
        dgain,
    )


def solution(mesh):
    placed = (
        P("dp", None, None),
        P(None, None, "dp", "mp"),
        P(None, "dp", None),
        P(None, "dp", "mp"),
        P(None, "mp", "dp"),
        P(),
        P(None, None, "mp"),
        P(None, "mp"),
        P(),
        P(),
        P(None, "mp"),
        P(None, "mp"),
        P(None, "mp"),
        P(None, "mp"),
        P("dp", None, None),
    )
    return jax.shard_map(
        per_device,
        mesh=mesh,
        in_specs=placed,
        out_specs=(
            P("dp", None, None),
            P("dp", None, None),
            P(None, None, "dp", "mp"),
            P(None, "dp", None),
            P(None, "dp", "mp"),
            P(None, "mp", "dp"),
            P(),
            P(None, None, "mp"),
            P(None, "mp"),
            P(),
            P(),
            P(None, "mp"),
            P(None, "mp"),
            P(None, "mp"),
            P(None, "mp"),
        ),
        check_vma=False,
    )
```

```python
import functools

import jax
import jax.numpy as jnp
from jax import lax
from jax.experimental import pallas as pl
from jax.experimental.pallas import tpu as pltpu
from jax.sharding import PartitionSpec as P

EPS = 1e-05
HIGH = lax.Precision.HIGHEST
CHUNK = 128
TAPS = 4
F32 = jnp.float32
BF16 = jnp.bfloat16


def dot_nn(a, b):
    return lax.dot_general(a, b, (((1,), (0,)), ((), ())), preferred_element_type=F32)


def dot_nt(a, b):
    return lax.dot_general(a, b, (((1,), (1,)), ((), ())), preferred_element_type=F32)


def dot_tn(a, b):
    return lax.dot_general(a, b, (((0,), (0,)), ((), ())), preferred_element_type=F32)


def sigmoid(v):
    return 0.5 * jnp.tanh(0.5 * v) + 0.5


def softplus(v):
    return jnp.maximum(v, 0.0) + jnp.log1p(jnp.exp(-jnp.abs(v)))


def lanes_of(shape):
    return lax.broadcasted_iota(jnp.int32, shape, 1)


def rows_of(shape):
    return lax.broadcasted_iota(jnp.int32, shape, 0)


def shifted_right(now, before, by):
    merged = jnp.where(lanes_of(now.shape) >= CHUNK - by, before, now)
    return pltpu.roll(merged, by, 1)


def shifted_left(now, after, by):
    merged = jnp.where(lanes_of(now.shape) < by, after, now)
    return pltpu.roll(merged, CHUNK - by, 1)


def decay_pieces(raw, bias, rate):
    step = softplus(raw + bias)
    upper = (rows_of((CHUNK, CHUNK)) <= lanes_of((CHUNK, CHUNK))).astype(F32)
    cum = lax.dot_general(
        step * rate, upper, (((1,), (0,)), ((), ())), precision=HIGH, preferred_element_type=F32
    )
    return step, cum


def transposed(a):
    rows = a.shape[0]
    padded = jnp.concatenate([a, jnp.zeros((CHUNK - rows, CHUNK), F32)], axis=0)
    return jnp.transpose(padded)


def forward_body(dims, flip_ref, z_ref, conv_ref, head_ref, row_ref, w_ref, sq_ref, y_ref, s_ref, act, tail, state, wide):
    inner, heads, width, states = dims
    chans = inner + 2 * states
    at = pl.program_id(0)

    @pl.when(at == 0)
    def _():
        tail[...] = jnp.zeros_like(tail)
        state[...] = jnp.zeros_like(state)
        for which in range(TAPS + 1):
            wide[which] = jnp.broadcast_to(conv_ref[:, which : which + 1], (chans, CHUNK))

    for row in range(0, chans, width):
        span = slice(row, row + width)
        now = z_ref[inner + row : inner + row + width, :].astype(F32)
        before = tail[span, :].astype(F32)
        conv = wide[TAPS, span, :] + wide[TAPS - 1, span, :] * now
        for by in range(1, TAPS):
            conv = conv + wide[TAPS - 1 - by, span, :] * shifted_right(now, before, by)
        act[span, :] = conv * sigmoid(conv)
    tail[...] = z_ref[inner : inner + chans, :]

    step, cum = decay_pieces(
        z_ref[inner + chans :, :].astype(F32), head_ref[:, 0:1], head_ref[:, 1:2]
    )
    cum_t = transposed(cum)
    key = act[inner : inner + states, :].astype(BF16)
    query = act[inner + states :, :].astype(BF16)
    scores = dot_tn(key, query)
    seen = rows_of((CHUNK, CHUNK)) <= lanes_of((CHUNK, CHUNK))
    grown = jnp.exp(cum)
    last = cum[:, CHUNK - 1 :]
    to_end = jnp.exp(last - cum) * step
    fade = jnp.broadcast_to(jnp.exp(last), cum.shape)
    squares = jnp.zeros((8, CHUNK), F32)
    s_ref[0] = state[...]
    for head in range(heads):
        span = slice(head * width, (head + 1) * width)
        gap = cum[head : head + 1, :] - cum_t[:, head : head + 1]
        mixing = (scores * jnp.exp(jnp.where(seen, gap, -1e30))).astype(BF16)
        x = act[span, :]
        held = state[span, :]
        scan = dot_nn((x * step[head : head + 1, :]).astype(BF16), mixing)
        scan = scan + grown[head : head + 1, :] * dot_nn(held.astype(BF16), query)
        y_ref[span, :] = scan
        state[span, :] = fade[head : head + 1, :] * held + dot_nt(
            (x * to_end[head : head + 1, :]).astype(BF16), key
        )
        gate = z_ref[span, :].astype(F32)
        gated = (scan + row_ref[span, 1:2] * x) * (gate * sigmoid(gate))
        squares = squares + jnp.sum((gated * gated).reshape(width // 8, 8, CHUNK), axis=0)
        w_ref[span, :] = (gated * row_ref[span, 0:1]).astype(BF16)
    sq_ref[...] = squares


def time_block(step, count, flip_ref):
    return lax.rem(step + flip_ref[0] * (count // 2), count)


def forward_mix(flip, z, conv_cols, head_cols, row_cols, dims):
    inner, heads, width, states = dims
    chans = inner + 2 * states
    rows, length = z.shape
    count = length // CHUNK
    here = lambda c, flip_ref: (0, time_block(c, count, flip_ref))
    whole = lambda c, flip_ref: (0, 0)
    return pl.pallas_call(
        functools.partial(forward_body, dims),
        grid_spec=pltpu.PrefetchScalarGridSpec(
            num_scalar_prefetch=1,
            grid=(count,),
            in_specs=[
                pl.BlockSpec((rows, CHUNK), here),
                pl.BlockSpec(conv_cols.shape, whole),
                pl.BlockSpec(head_cols.shape, whole),
                pl.BlockSpec(row_cols.shape, whole),
            ],
            out_specs=[
                pl.BlockSpec((inner, CHUNK), here),
                pl.BlockSpec((8, CHUNK), here),
                pl.BlockSpec((inner, CHUNK), here),
                pl.BlockSpec((1, inner, states), lambda c, flip_ref: (c, 0, 0)),
            ],
            scratch_shapes=[
                pltpu.VMEM((chans, CHUNK), F32),
                pltpu.VMEM((chans, CHUNK), BF16),
                pltpu.VMEM((inner, states), F32),
                pltpu.VMEM((TAPS + 1, chans, CHUNK), F32),
            ],
        ),
        out_shape=[
            jax.ShapeDtypeStruct((inner, length), BF16),
            jax.ShapeDtypeStruct((8, length), F32),
            jax.ShapeDtypeStruct((inner, length), F32),
            jax.ShapeDtypeStruct((count, inner, states), F32),
        ],
        cost_estimate=pl.CostEstimate(
            flops=2 * length * inner * (CHUNK + 2 * states) * 2,
            bytes_accessed=rows * length * 2 + inner * length * 6 + count * inner * states * 4,
            transcendentals=length * heads * CHUNK,
        ),
        name="mix_forward",
    )(flip, z, conv_cols, head_cols, row_cols)


def backward_body(
    dims, flip_ref, z_ref, zp_ref, dw_ref, r_ref, y_ref, s_ref, conv_ref, head_ref, row_ref,
    dz_ref, chan_ref, inner_ref, hsum_ref,
    act, slope, shifts, later, snext, dstate, dact, wide, acc_c, acc_i, acc_h, prod,
):
    inner, heads, width, states = dims
    chans = inner + 2 * states
    hrows = head_ref.shape[0]
    at = pl.program_id(0)
    total = pl.num_programs(0)

    @pl.when(at == 0)
    def _():
        later[...] = jnp.zeros_like(later)
        snext[...] = jnp.zeros_like(snext)
        dstate[...] = jnp.zeros_like(dstate)
        acc_c[...] = jnp.zeros_like(acc_c)
        acc_i[...] = jnp.zeros_like(acc_i)
        acc_h[...] = jnp.zeros_like(acc_h)
        for which in range(TAPS + 1):
            wide[which] = jnp.broadcast_to(conv_ref[:, which : which + 1], (chans, CHUNK))

    started = jnp.where(at == total - 1, 0.0, 1.0)
    for row in range(0, chans, width):
        span = slice(row, row + width)
        now = z_ref[inner + row : inner + row + width, :].astype(F32)
        before = zp_ref[inner + row : inner + row + width, :].astype(F32) * started
        conv = wide[TAPS, span, :] + wide[TAPS - 1, span, :] * now
        for by in range(1, TAPS):
            moved = shifted_right(now, before, by)
            shifts[by - 1, span, :] = moved
            conv = conv + wide[TAPS - 1 - by, span, :] * moved
        sig = sigmoid(conv)
        out = conv * sig
        act[span, :] = out
        slope[span, :] = sig + out * (1.0 - sig)

    raw = z_ref[inner + chans :, :].astype(F32) + head_ref[:, 0:1]
    rate = head_ref[:, 1:2]
    step, cum = decay_pieces(raw, 0.0, rate)
    cum_t = transposed(cum)
    key = act[inner : inner + states, :].astype(BF16)
    query = act[inner + states :, :].astype(BF16)
    scores = dot_tn(key, query)
    seen = rows_of((CHUNK, CHUNK)) <= lanes_of((CHUNK, CHUNK))
    grown = jnp.exp(cum)
    last = cum[:, CHUNK - 1 :]
    to_end = jnp.exp(last - cum)
    fade = jnp.broadcast_to(jnp.exp(last), cum.shape)
    dscores = jnp.zeros((CHUNK, CHUNK), F32)
    dkey = jnp.zeros((states, CHUNK), F32)
    dquery = jnp.zeros((states, CHUNK), F32)
    weight_row = r_ref[0:1, :]
    for head in range(heads):
        span = slice(head * width, (head + 1) * width)
        one = slice(head, head + 1)
        x = act[span, :]
        gate = z_ref[span, :].astype(F32)
        sg = sigmoid(gate)
        sgate = gate * sg
        scan = y_ref[span, :]
        y = scan + row_ref[span, 1:2] * x
        gated = y * sgate
        dw = dw_ref[span, :].astype(F32)
        dgated = dw * row_ref[span, 0:1] - weight_row * gated
        acc_i[0, span, :] += dw * gated
        dy = dgated * sgate
        acc_i[1, span, :] += dy * x
        dz_ref[span, :] = (dgated * y * (sg + sgate * (1.0 - sg))).astype(BF16)

        gap = cum[one, :] - cum_t[:, one]
        decay = jnp.exp(jnp.where(seen, gap, -1e30))
        mixing = (scores * decay).astype(BF16)
        dyb = dy.astype(BF16)
        xd = x * step[one, :]
        xdb = xd.astype(BF16)
        dscores = dscores + dot_tn(xdb, dyb) * decay
        dstb = dstate[span, :].astype(BF16)
        dxd = dot_nt(dyb, mixing) + to_end[one, :] * dot_nn(dstb, key)
        wxd = (xd * to_end[one, :]).astype(BF16)
        edy = (dy * grown[one, :]).astype(BF16)
        dkey = dkey + dot_tn(dstb, wxd)
        dquery = dquery + dot_tn(s_ref[0, span, :].astype(BF16), edy)
        prod[0, one, :] = jnp.sum(
            dyb.astype(F32) * scan - xdb.astype(F32) * dxd, axis=0, keepdims=True
        )
        prod[1, one, :] = jnp.sum(x * dxd, axis=0, keepdims=True)
        held = dstate[span, :]
        prod[2, one, :] = jnp.sum(snext[span, :] * held, axis=0, keepdims=True)
        dstate[span, :] = fade[one, :] * held + dot_nt(edy, query)
        dact[span, :] = step[one, :] * dxd + row_ref[span, 1:2] * dy
    snext[...] = s_ref[0]
    dsb = dscores.astype(BF16)
    dact[inner : inner + states, :] = dkey + dot_nt(query, dsb)
    dact[inner + states :, :] = dquery + dot_nn(key, dsb)

    live = rows_of((hrows, CHUNK)) < heads
    lower = (rows_of((CHUNK, CHUNK)) >= lanes_of((CHUNK, CHUNK))).astype(F32)
    zero = jnp.zeros((hrows, CHUNK), F32)
    dla = lax.dot_general(
        jnp.where(live, prod[0], zero), lower, (((1,), (0,)), ((), ())), precision=HIGH,
        preferred_element_type=F32,
    ) + jnp.sum(jnp.where(live, prod[2], zero), axis=1, keepdims=True)
    dstep = jnp.where(live, prod[1], zero) + rate * dla
    draw = dstep * sigmoid(raw)
    acc_h[0] += draw
    acc_h[1] += step * dla
    dz_ref[inner + chans :, :] = draw.astype(BF16)

    for row in range(0, chans, width):
        span = slice(row, row + width)
        dconv = dact[span, :] * slope[span, :]
        acc_c[TAPS, span, :] += dconv
        acc_c[TAPS - 1, span, :] += dconv * z_ref[inner + row : inner + row + width, :].astype(F32)
        back = wide[TAPS - 1, span, :] * dconv
        after = later[span, :]
        for by in range(1, TAPS):
            acc_c[TAPS - 1 - by, span, :] += dconv * shifts[by - 1, span, :]
            back = back + wide[TAPS - 1 - by, span, :] * shifted_left(dconv, after, by)
        later[span, :] = dconv
        dz_ref[inner + row : inner + row + width, :] = back.astype(BF16)

    @pl.when(at == total - 1)
    def _():
        ones = jnp.ones((8, CHUNK), F32)

        def sums(block):
            return lax.dot_general(
                ones, block, (((1,), (1,)), ((), ())), precision=HIGH, preferred_element_type=F32
            )

        for which in range(TAPS + 1):
            chan_ref[which] = sums(acc_c[which])
        for which in range(2):
            inner_ref[which] = sums(acc_i[which])
            hsum_ref[which] = acc_h[which]


def backward_mix(flip, z, dw, r, y, s, conv_cols, head_cols, row_cols, dims):
    inner, heads, width, states = dims
    chans = inner + 2 * states
    rows, length = z.shape
    hrows = head_cols.shape[0]
    count = length // CHUNK
    back = lambda c, flip_ref: (0, time_block(count - 1 - c, count, flip_ref))
    whole = lambda c, flip_ref: (0, 0)
    whole3 = lambda c, flip_ref: (0, 0, 0)
    return pl.pallas_call(
        functools.partial(backward_body, dims),
        grid_spec=pltpu.PrefetchScalarGridSpec(
            num_scalar_prefetch=1,
            grid=(count,),
            in_specs=[
                pl.BlockSpec((rows, CHUNK), back),
                pl.BlockSpec(
                    (rows, CHUNK),
                    lambda c, flip_ref: (
                        0,
                        time_block(jnp.maximum(count - 2 - c, 0), count, flip_ref),
                    ),
                ),
                pl.BlockSpec((inner, CHUNK), back),
                pl.BlockSpec((8, CHUNK), back),
                pl.BlockSpec((inner, CHUNK), back),
                pl.BlockSpec((1, inner, states), lambda c, flip_ref: (count - 1 - c, 0, 0)),
                pl.BlockSpec(conv_cols.shape, whole),
                pl.BlockSpec(head_cols.shape, whole),
                pl.BlockSpec(row_cols.shape, whole),
            ],
            out_specs=[
                pl.BlockSpec((rows, CHUNK), back),
                pl.BlockSpec((TAPS + 1, 8, chans), whole3),
                pl.BlockSpec((2, 8, inner), whole3),
                pl.BlockSpec((2, hrows, CHUNK), whole3),
            ],
            scratch_shapes=[
                pltpu.VMEM((chans, CHUNK), F32),
                pltpu.VMEM((chans, CHUNK), F32),
                pltpu.VMEM((TAPS - 1, chans, CHUNK), F32),
                pltpu.VMEM((chans, CHUNK), F32),
                pltpu.VMEM((inner, states), F32),
                pltpu.VMEM((inner, states), F32),
                pltpu.VMEM((chans, CHUNK), F32),
                pltpu.VMEM((TAPS + 1, chans, CHUNK), F32),
                pltpu.VMEM((TAPS + 1, chans, CHUNK), F32),
                pltpu.VMEM((2, inner, CHUNK), F32),
                pltpu.VMEM((2, hrows, CHUNK), F32),
                pltpu.VMEM((3, hrows, CHUNK), F32),
            ],
        ),
        out_shape=[
            jax.ShapeDtypeStruct((rows, length), BF16),
            jax.ShapeDtypeStruct((TAPS + 1, 8, chans), F32),
            jax.ShapeDtypeStruct((2, 8, inner), F32),
            jax.ShapeDtypeStruct((2, hrows, CHUNK), F32),
        ],
        cost_estimate=pl.CostEstimate(
            flops=4 * length * inner * (CHUNK + 2 * states) * 2,
            bytes_accessed=rows * length * 6 + inner * length * 6 + count * inner * states * 4,
            transcendentals=length * heads * CHUNK,
        ),
        name="mix_backward",
    )(flip, z, z, dw, r, y, s, conv_cols, head_cols, row_cols)


def per_device(
    block_input,
    zx_weight,
    bc_weight,
    dt_weight,
    out_weight,
    norm_gain,
    inner_conv,
    inner_conv_bias,
    state_conv,
    state_conv_bias,
    dt_bias,
    a_log,
    d_skip,
    gated_gain,
    cotangent,
):
    layers, _, shard, inner = zx_weight.shape
    sequences, length, model = block_input.shape
    pair = bc_weight.shape[2]
    states = pair // 2
    heads = dt_weight.shape[2]
    width = inner // heads
    inner_total = inner * lax.axis_size("mp")
    hrows = -(-heads // 16) * 16
    chans = inner + pair
    dims = (inner, heads, width, states)

    in_full, out_full, cols = [], [], []
    for layer in range(layers):
        packed = jnp.concatenate(
            [
                zx_weight[layer, 0],
                zx_weight[layer, 1],
                bc_weight[layer],
                jnp.pad(dt_weight[layer], ((0, 0), (0, hrows - heads))),
            ],
            axis=1,
        )
        in_full.append(lax.all_gather(packed, "dp", axis=0, tiled=True))
        taps = jnp.concatenate([inner_conv[layer], state_conv[layer]], axis=1)
        offset = jnp.concatenate([inner_conv_bias[layer], state_conv_bias[layer]])
        conv_cols = jnp.pad(jnp.concatenate([taps, offset[None]], axis=0), ((0, 3), (0, 0))).T
        head_cols = jnp.pad(
            jnp.stack([dt_bias[layer], -jnp.exp(a_log[layer])], axis=1),
            ((0, hrows - heads), (0, 6)),
        )
        row_cols = jnp.pad(
            jnp.stack([gated_gain[layer], jnp.repeat(d_skip[layer], width)], axis=1),
            ((0, 0), (0, 6)),
        )
        cols.append((conv_cols, head_cols, row_cols))

    group = lax.axis_size("mp")
    ranks = lax.axis_size("dp")
    rank = lax.axis_index("mp")
    core = lax.rem(rank, 2)
    half = length // 2
    flip = core.astype(jnp.int32).reshape(1)

    def swap(value, bit, axis="mp"):
        size = group if axis == "mp" else ranks
        return lax.ppermute(value, axis, [(at, at ^ bit) for at in range(size)])

    def own_first(value):
        mine = lax.dynamic_slice_in_dim(value, core * half, half)
        other = lax.dynamic_slice_in_dim(value, (1 - core) * half, half)
        return jnp.concatenate([mine, other], axis=0)

    def in_order(mine):
        other = swap(mine, 1)
        return jnp.where(
            core == 0,
            jnp.concatenate([mine, other], axis=0),
            jnp.concatenate([other, mine], axis=0),
        )

    def joined(mine):
        return jnp.concatenate([mine, swap(mine, 1)], axis=0)

    minor = 1
    while minor * minor * 4 <= ranks:
        minor *= 2
    major = ranks // minor
    place = lax.axis_index("dp")
    major_at, minor_at = place // minor, lax.rem(place, minor)

    def shift(value, up, across):
        pairs = [
            (at, (at // minor + up) % major * minor + (at % minor + across) % minor)
            for at in range(ranks)
        ]
        return lax.ppermute(value, "dp", pairs)

    def gather_major(piece):
        return [piece] + [shift(piece, up, 0) for up in range(1, major)]

    def gather_minor(pieces):
        rows = pieces[0].shape[0]
        full = jnp.zeros((rows * ranks,) + pieces[0].shape[1:], pieces[0].dtype)
        for across in range(minor):
            for up, piece in enumerate(pieces):
                piece = shift(piece, 0, across) if across else piece
                owner = lax.rem(major_at + major - up, major) * minor
                owner = owner + lax.rem(minor_at + minor - across, minor)
                full = lax.dynamic_update_slice_in_dim(full, piece, owner * rows, 0)
        return full

    def scatter_minor(terms):
        blocks = terms.reshape(major, minor, -1, terms.shape[-1])
        pick = lambda at: lax.dynamic_index_in_dim(blocks, at, 1, keepdims=False)
        total = pick(minor_at).astype(F32)
        for across in range(1, minor):
            total = total + shift(pick(lax.rem(minor_at + across, minor)), 0, across).astype(F32)
        return total.astype(BF16)

    def scatter_major(blocks):
        pick = lambda at: lax.dynamic_index_in_dim(blocks, at, 0, keepdims=False)
        total = pick(major_at).astype(F32)
        for up in range(1, major):
            total = total + shift(pick(lax.rem(major_at + up, major)), up, 0).astype(F32)
        return total

    def tie(*values):
        return lax.optimization_barrier(values)

    def send_own(theirs, mine):
        sent = (mine.astype(F32) + swap(theirs, 1).astype(F32)).astype(BF16)
        return sent, (swap(sent, 2) if group > 2 else jnp.zeros_like(sent))

    def sum_own(sent, got):
        total = sent.astype(F32) + got.astype(F32)
        bit = 4
        while bit < group:
            sent = total.astype(BF16)
            total = sent.astype(F32) + swap(sent, bit).astype(F32)
            bit *= 2
        return total

    def sum_rows(values):
        total = values[:half]
        for bits in range(1, group):
            total = total + swap(values[half:] if bits % 2 else values[:half], bits)
        return total

    def sum_all(value, axis):
        bit = 1
        while bit < (group if axis == "mp" else ranks):
            value = (value.astype(F32) + swap(value, bit, axis).astype(F32)).astype(value.dtype)
            bit *= 2
        return value

    def normalized(layer, hidden):
        root = lax.rsqrt(jnp.mean(hidden * hidden, axis=-1) + EPS)
        return root, (hidden * root[:, None] * norm_gain[layer][None, :]).astype(BF16)

    def forward_unit(layer, normed):
        z = jnp.einsum("df,td->ft", in_full[layer], normed, preferred_element_type=F32).astype(BF16)
        weighted, squares, scan, held = forward_mix(flip, z, *cols[layer], dims)
        theirs, mine = (
            jnp.einsum("it,di->td", part, out_full[layer], preferred_element_type=F32).astype(BF16)
            for part in (weighted[:, half:], weighted[:, :half])
        )
        scale = lax.rsqrt(sum_rows(jnp.sum(squares, axis=0)) / inner_total + EPS)
        return (normed, z, weighted, scan, held, scale), theirs, mine

    def backward_head(scale, grad, summed):
        dsummed = joined((scale[:, None] * grad).astype(BF16))
        dscale = jnp.sum(grad * summed, axis=-1)
        return dsummed, joined(dscale * scale**3 / inner_total)

    def backward_unit(layer, saved, dsummed, ratio):
        _, z, _, scan, held, _ = saved
        dweighted = jnp.einsum(
            "td,di->it", dsummed, out_full[layer], preferred_element_type=F32
        ).astype(BF16)
        return backward_mix(
            flip, z, dweighted, jnp.broadcast_to(ratio, (8, length)), scan, held, *cols[layer], dims
        )

    def backward_out(layer, dz):
        return [
            jnp.einsum("ft,df->td", part, in_full[layer], preferred_element_type=F32).astype(BF16)
            for part in (dz[:, half:], dz[:, :half])
        ]

    def backward_tail(layer, hidden, root, grad, dnormed):
        unit = hidden * root[:, None]
        dnorm = jnp.sum(dnormed * unit, axis=0)
        back = dnormed * norm_gain[layer][None, :]
        grad = grad + root[:, None] * (
            back - unit * jnp.mean(back * unit, axis=-1, keepdims=True)
        )
        return grad, dnorm

    def out_term(dsummed_of, saved_of):
        return sum(
            jnp.einsum("td,it->di", top, saved[2], preferred_element_type=F32)
            for top, saved in zip(dsummed_of, saved_of)
        ).astype(BF16)

    def in_term(saved_of, dz_of, rows):
        return sum(
            jnp.einsum("td,ft->df", saved[0], dz[rows], preferred_element_type=F32)
            for saved, dz in zip(saved_of, dz_of)
        ).astype(BF16)

    everyone = range(sequences)
    top = layers - 1
    hidden = [
        [lax.dynamic_slice_in_dim(block_input[seq], core * half, half).astype(F32)]
        for seq in everyone
    ]
    roots = [[normalized(0, hidden[seq][0])[0]] for seq in everyone]
    normed = [normalized(0, own_first(block_input[seq]).astype(F32))[1] for seq in everyone]
    summed = [[] for _ in everyone]
    saved = [[] for _ in range(layers)]
    flying = [None] * sequences
    newest = None

    def landed(seq):
        sent, got = flying[seq]
        got, _ = tie(got, newest)
        return sum_own(sent, got)

    pieces = gather_major(out_weight[0].T)
    for layer in range(layers):
        for seq in everyone:
            if layer:
                summed[seq].append(landed(seq))
                scale = saved[layer - 1][seq][5]
                hidden[seq].append(hidden[seq][-1] + scale[:, None] * summed[seq][-1])
                root, mine = normalized(layer, hidden[seq][-1])
                roots[seq].append(root)
                normed[seq] = joined(mine)
            elif seq:
                normed[seq], _ = tie(normed[seq], newest)
            if seq == 0:
                normed[seq], *pieces = tie(normed[seq], *pieces)
                out_full.append(gather_minor(pieces))
                if layer < top:
                    piece, _ = tie(out_weight[layer + 1].T, in_full[layer])
                    pieces = gather_major(piece)
            kept, theirs, newest = forward_unit(layer, normed[seq])
            saved[layer].append(kept)
            flying[seq] = send_own(theirs, newest)

    grad = [
        lax.dynamic_slice_in_dim(cotangent[seq], core * half, half).astype(F32)
        for seq in everyone
    ]
    outputs = []
    gate_grads, rest_grads = [None] * layers, [None] * layers
    out_grads, small_grads = [None] * layers, [None] * layers
    dnorms = [[None] * sequences for _ in range(layers)]
    dsummed = [[None] * sequences for _ in range(layers)]
    for layer in reversed(range(layers)):
        dz_of, smalls = [], []
        for seq in everyone:
            arrived = landed(seq)
            scale = saved[layer][seq][5]
            if layer == top:
                summed[seq].append(arrived)
                outputs.append(in_order((hidden[seq][-1] + scale[:, None] * arrived).astype(BF16)))
            else:
                grad[seq], dnorms[layer + 1][seq] = backward_tail(
                    layer + 1, hidden[seq][layer + 1], roots[seq][layer + 1], grad[seq], arrived
                )
            dsummed[layer][seq], ratio = backward_head(scale, grad[seq], summed[seq][layer])
            if seq == sequences - 1:
                term = out_term(dsummed[layer], saved[layer])
                dsummed[layer][seq], term = tie(dsummed[layer][seq], term)
                out_grads[layer] = scatter_major(scatter_minor(term))
            dz, *small = backward_unit(layer, saved[layer][seq], dsummed[layer][seq], ratio)
            dz_of.append(dz)
            smalls.append(small)
            theirs, newest = backward_out(layer, dz)
            flying[seq] = send_own(theirs, newest)
        if layer:
            dz_of[-1], _ = tie(dz_of[-1], newest)
            newest = in_term(saved[layer], dz_of, slice(None))
            whole = lax.psum_scatter(newest, "dp", scatter_dimension=0, tiled=True)
            gate_grads[layer], rest_grads[layer] = whole[:, :inner], whole[:, inner:]
        else:
            blocks = scatter_minor(in_term(saved[layer], dz_of, slice(0, inner)))
            gate_grads[layer] = scatter_major(blocks)
            rest = in_term(saved[layer], dz_of, slice(inner, None))
            rest, *rest_grads[1:] = tie(rest, *rest_grads[1:])
            rest_grads[layer] = lax.psum_scatter(rest, "dp", scatter_dimension=0, tiled=True)
        small_grads[layer] = [sum(parts) for parts in zip(*smalls)]
    for seq in everyone:
        grad[seq], dnorms[0][seq] = backward_tail(
            0, hidden[seq][0], roots[seq][0], grad[seq], sum_own(*flying[seq])
        )
    outputs = jnp.stack(outputs)
    input_grad = jnp.stack([in_order(item.astype(BF16)).astype(F32) for item in grad])

    out_grad = jnp.stack([item.T for item in out_grads]).astype(F32)
    zx_grad = jnp.stack(
        [
            jnp.stack([gate.astype(F32), rest[:, :inner].astype(F32)])
            for gate, rest in zip(gate_grads, rest_grads)
        ]
    )
    dt_grad = jnp.stack(
        [rest[:, inner + pair : inner + pair + heads].astype(F32) for rest in rest_grads]
    )
    bc_grad = jnp.stack(
        [sum_all(rest[:, inner : inner + pair], "mp").astype(F32) for rest in rest_grads]
    )
    dnorm = jnp.stack([sum(parts) for parts in dnorms])
    dchan = jnp.stack([item[0][:, 0] for item in small_grads])
    dinner = jnp.stack([item[1][:, 0] for item in small_grads])
    dheads = jnp.stack([jnp.sum(item[2], axis=-1)[:, :heads] for item in small_grads])
    dskip = jnp.sum(dinner[:, 1].reshape(layers, heads, width), axis=-1)
    dlog = dheads[:, 1] * -jnp.exp(a_log)
    parts = [
        dnorm,
        dchan[:, :, inner:].reshape(layers, -1),
        dchan[:, :, :inner].reshape(layers, -1),
        dinner[:, 0],
        dheads[:, 0],
        dlog,
        dskip,
    ]
    spots, at = [], 0
    for part in parts[:-1]:
        at += part.shape[1]
        spots.append(at)
    vector = sum_all(jnp.concatenate(parts, axis=1), "dp")
    shared = sum_all(vector[:, : spots[1]], "mp")
    dnorm = shared[:, : spots[0]] * (2.0 / group)
    dstate = shared[:, spots[0] :].reshape(layers, TAPS + 1, pair)
    _, _, dlocal, dgain, dbias, dlog, dskip = jnp.split(vector, spots, axis=1)
    dlocal = dlocal.reshape(layers, TAPS + 1, inner)
    return (
        outputs,
        input_grad,
        zx_grad,
        bc_grad,
        dt_grad,
        out_grad,
        dnorm,
        dlocal[:, :TAPS],
        dlocal[:, TAPS],
        dstate[:, :TAPS],
        dstate[:, TAPS],
        dbias,
        dlog,
        dskip,
        dgain,
    )


def solution(mesh):
    placed = (
        P("dp", None, None),
        P(None, None, "dp", "mp"),
        P(None, "dp", None),
        P(None, "dp", "mp"),
        P(None, "mp", "dp"),
        P(),
        P(None, None, "mp"),
        P(None, "mp"),
        P(),
        P(),
        P(None, "mp"),
        P(None, "mp"),
        P(None, "mp"),
        P(None, "mp"),
        P("dp", None, None),
    )
    return jax.shard_map(
        per_device,
        mesh=mesh,
        in_specs=placed,
        out_specs=(
            P("dp", None, None),
            P("dp", None, None),
            P(None, None, "dp", "mp"),
            P(None, "dp", None),
            P(None, "dp", "mp"),
            P(None, "mp", "dp"),
            P(),
            P(None, None, "mp"),
            P(None, "mp"),
            P(),
            P(),
            P(None, "mp"),
            P(None, "mp"),
            P(None, "mp"),
            P(None, "mp"),
        ),
        check_vma=False,
    )
```
